32 devices in a mesh: dp: 8 (over z, x), seq: 4 (over y, core).
Axes of the slice: x: 2, y: 2, z: 4, core: 2. Of those that a mesh axis runs over, the one named last changes fastest.
Arguments:
- hidden: bfloat16 [8, 4096, 4096], P('dp', 'seq'), may hold values from -6 to 6
- value_weight: bfloat16 [4096, 64], replicated, may hold values from -0.09375 to 0.09375
- value_bias: float32 [64], replicated, may hold values from -1 to 1
- returns: float32 [8, 4096], P('dp', 'seq'), may hold values from -12 to 12, as said below
- task_bins: int32 [8, 4096], P('dp', 'seq'), may hold values from 0 to 63
- loss_mask: int32 [8, 4096], P('dp', 'seq'), may hold values 0 or 1
Outputs:
- targets: float32 [8, 4096], P('dp', 'seq')
- weight_grad: float32 [4096, 64], replicated
- bias_grad: float32 [64], replicated
The draws below stay inside these ranges and needn't reach their ends.
Inputs may be any that keep to these rules, and one draw needn't show every extreme that they name: The returns of one rollout share a level and a trend along positions.
All inputs are finite; a program needn't handle non-finite values.
Results may differ from the reference program's by a relative error of at most 0.00083.
Values sent between devices are 32-bit elements.
A program may use at most 64 MiB of HBM per device.

```python
import math
import jax
import jax.numpy as jnp
import numpy as np
from jax import lax

D = 4096
NB = 64
ROLLOUTS = 8
LENGTH = 4096


def draw_returns(key, part):
    keys = jax.random.split(key, 4)
    level = jax.random.uniform(keys[0], (ROLLOUTS, 1), jnp.float32, -3.0, 3.0)
    noise = jnp.clip(jax.random.normal(keys[2], (ROLLOUTS, LENGTH), jnp.float32), -3.0, 3.0)
    trend = jax.random.uniform(keys[1], (ROLLOUTS, 1), jnp.float32, -2.0, 2.0)
    spread = jnp.exp(jax.random.uniform(keys[3], (ROLLOUTS, 1), jnp.float32, math.log(0.5), math.log(2.0)))
    position = jnp.arange(LENGTH, dtype=jnp.float32) / LENGTH
    return level + trend * position[None, :] + noise * spread


def plant(result, key, smallest, largest):
    extent = result.shape
    spot = [jax.random.randint(jax.random.fold_in(key, axis), (), 0, extent[axis]) for axis in range(len(extent))]
    result = result.at[tuple(spot)].set(smallest)
    longest = extent.index(max(extent))
    spot[longest] = (spot[longest] + 1) % extent[longest]
    return result.at[tuple(spot)].set(largest)


def steps_of(own_key, extent, shards, low, largest):
    factor_of, own = 1.0, jax.random.fold_in(own_key, 6)
    for axis_at, shards_of in shards:
        heights = jnp.exp(jax.random.uniform(jax.random.fold_in(own, axis_at), (shards_of,), jnp.float32, low / len(shards), largest / len(shards)))
        factor_of = factor_of * jnp.repeat(heights, extent[axis_at] // shards_of).reshape([-1 if axis == axis_at else 1 for axis in range(len(extent))])
    return factor_of


def cumulative_ranks(number_of, skew):
    weights = [(1 << 20) // math.isqrt(grade ** skew) + 1 for grade in range(1, number_of + 1)]
    scale = 1 + sum(weights) // (1 << 30)
    return np.cumsum(np.array([max(1, weight // scale) for weight in weights]))


def skewed_ids(key, shape, number_of, skew):
    grid = cumulative_ranks(number_of, skew)
    pick = jax.random.randint(jax.random.fold_in(key, 1), shape, 0, int(grid[number_of - 1]))
    grade = jnp.searchsorted(jnp.asarray(grid, jnp.int32), pick, side="right")
    return jax.random.permutation(jax.random.fold_in(key, 2), number_of)[grade].astype(jnp.int32)


def centred(own_key, extent, scale, most, shards=(), kind=jnp.bfloat16):
    drawn = scale * jax.random.normal(own_key, extent, jnp.float32)
    if shards:
        drawn = drawn * steps_of(own_key, extent, shards, -0.22, 0.18)
    return jnp.clip(drawn, -most, most).astype(kind)


def setup_inputs(seed: int = 0) -> dict:
    arg_keys = jax.random.split(jax.random.key(seed), 7)
    hidden = centred(arg_keys[0], (ROLLOUTS, LENGTH, D), 1.0, 6.0, ((0, 8), (1, 4)))
    value_weight = centred(arg_keys[1], (D, NB), D ** -0.5, 0.09375)
    value_bias = jnp.clip(jax.random.uniform(arg_keys[2], (NB,), jnp.float32, -1.0, 1.0), -1.0, 1.0)
    returns = draw_returns(jax.random.fold_in(arg_keys[6], 71), 0)
    task_bins = plant(skewed_ids(arg_keys[4], (ROLLOUTS, LENGTH), NB, 2), jax.random.fold_in(arg_keys[4], 3), 0, NB - 1).astype(jnp.int32)
    loss_mask = plant((jax.random.randint(arg_keys[5], (ROLLOUTS, LENGTH), 0, 4) < 3).astype(jnp.int32), jax.random.fold_in(arg_keys[5], 1), 0, 1)
    return {"hidden": hidden, "value_weight": value_weight, "value_bias": value_bias, "returns": returns, "task_bins": task_bins, "loss_mask": loss_mask}


def reference(hidden, value_weight, value_bias, returns, task_bins, loss_mask):
    bins_iota = jnp.arange(NB, dtype=jnp.int32)
    chosen = (task_bins[..., None] == bins_iota).astype(jnp.float32)
    onehot = chosen * loss_mask[..., None].astype(jnp.float32)
    counts = lax.optimization_barrier(jnp.sum(onehot, axis=(0, 1)))
    floor_counts = jnp.maximum(counts, 1.0)
    means = lax.optimization_barrier(jnp.sum(onehot * returns[..., None], axis=(0, 1))) / floor_counts
    deviation = returns[..., None] - means
    second = lax.optimization_barrier(jnp.sum(onehot * deviation * deviation, axis=(0, 1)))
    spread = jnp.sqrt(second / floor_counts + 0.1)
    targets = lax.optimization_barrier(jnp.sum(chosen * (deviation / spread), axis=-1))

    def rollout_step(running, slices):
        states, target_row, chosen_row, valid = slices
        scores = jnp.dot(states, value_weight, preferred_element_type=jnp.float32)
        predicted = lax.optimization_barrier(jnp.sum((scores + value_bias) * chosen_row, axis=-1))
        slope = valid * jnp.clip(predicted - target_row, -1.0, 1.0) / ROLLOUTS
        coefficient = chosen_row * slope[:, None]
        weight_part = lax.dot_general(states, coefficient.astype(jnp.bfloat16), (((0,), (0,)), ((), ())), preferred_element_type=jnp.float32)
        return ((running[0] + weight_part, running[1] + lax.optimization_barrier(jnp.sum(coefficient, axis=0))), None)
    start = (jnp.zeros((D, NB), jnp.float32), jnp.zeros((NB,), jnp.float32))
    (weight_grad, bias_grad), unused = lax.scan(rollout_step, start, (hidden, targets, chosen, loss_mask.astype(jnp.float32)))
    return (targets, weight_grad, bias_grad)
```

```python
import functools

import jax
import jax.numpy as jnp
from jax import lax
from jax.experimental import pallas as pl
from jax.experimental.pallas import tpu as pltpu
from jax.sharding import PartitionSpec as P

MESH = pl.DeviceIdType.MESH
LANES = 128
TOKENS = 256


def split_in_two(n):
    return 2 if n % 2 == 0 else 1


def plan(ndp, nseq, tiles):
    core, x = split_in_two(nseq), split_in_two(ndp)
    sizes = {"core": core, "y": nseq // core, "x": x, "z": ndp // x}
    streams = 4
    while streams > 1 and (tiles % (streams * ndp * nseq) or tiles % (streams * core * 8)):
        streams //= 2
    return sizes, streams


def kernel(ndp, nseq, rollouts, sizes, streams, hidden, weight, bias, returns, bins, mask,
           targets, grad, bias_grad, *scratch):
    (held, acc, whole, coef, predicted, turned, small, small_in, row_in, hid_sem,
     small_send, small_recv) = scratch[:12]
    stage_scratch = scratch[12:]
    tasks, width = weight.shape
    tokens = hidden.shape[0]
    tiles = acc.shape[0]
    dp, seq = lax.axis_index("dp"), lax.axis_index("seq")
    core, y = lax.rem(seq, sizes["core"]), lax.div(seq, sizes["core"])
    x, z = lax.rem(dp, sizes["x"]), lax.div(dp, sizes["x"])

    barrier = pltpu.get_barrier_semaphore()
    for r in range(1, nseq):
        pl.semaphore_signal(barrier, inc=1, device_id={"seq": lax.rem(seq + r, nseq)}, device_id_type=MESH)
    for r in range(1, ndp):
        pl.semaphore_signal(barrier, inc=1, device_id={"dp": lax.rem(dp + r, ndp)}, device_id_type=MESH)

    loads = []
    for j in range(tokens // TOKENS):
        rows = pl.ds(j * TOKENS, TOKENS)
        loads.append(pltpu.make_async_copy(hidden.at[rows], held.at[rows], hid_sem.at[j]))
        loads[-1].start()

    def peer(name, r):
        n = sizes[name]
        if name == "core":
            return {"seq": y * n + lax.rem(core + r, n)}
        if name == "y":
            return {"seq": lax.rem(y + r, n) * sizes["core"] + core}
        if name == "x":
            return {"dp": z * n + lax.rem(x + r, n)}
        return {"dp": lax.rem(z + r, n) * sizes["x"] + x}

    place = {"core": core, "y": y, "x": x, "z": z}

    def small_start(k, axis):
        n, me = (nseq, seq) if axis == "seq" else (ndp, dp)
        landing = small_in if axis == "seq" else row_in
        base = 0 if axis == "seq" else nseq - 1
        copies = []
        for r in range(1, n):
            copies.append(pltpu.make_async_remote_copy(
                src_ref=small.at[2 * k + (axis == "dp")], dst_ref=landing.at[k, r - 1],
                send_sem=small_send.at[k, base + r - 1], recv_sem=small_recv.at[k, base + r - 1],
                device_id={axis: lax.rem(me + r, n)}, device_id_type=MESH))
            copies[-1].start()
        return copies

    def small_finish(k, axis, copies):
        landing = small_in if axis == "seq" else row_in
        total = small[2 * k + (axis == "dp")]
        for r, copy in enumerate(copies):
            copy.wait()
            total = total + landing[k, r]
        return total

    def onehot_of(block):
        chosen = bins[:, block] == lax.broadcasted_iota(jnp.int32, (tasks, LANES), 0)
        return chosen, mask[:, block].astype(jnp.float32)

    blocks = [pl.ds(k * LANES, LANES) for k in range(tokens // LANES)]
    counted = summed = squared = jnp.zeros((tasks, LANES), jnp.float32)
    for block in blocks:
        chosen, valid = onehot_of(block)
        value = returns[:, block]
        counted = counted + jnp.where(chosen, valid, 0.0)
        summed = summed + jnp.where(chosen, valid * value, 0.0)
        squared = squared + jnp.where(chosen, valid * value * value, 0.0)
    lane = lax.broadcasted_iota(jnp.int32, (tasks, LANES), 1)
    columns = jnp.zeros((tasks, LANES), jnp.float32)
    for k, part in enumerate((counted, summed, squared)):
        columns = jnp.where(lane == k, jnp.sum(part, axis=1, keepdims=True), columns)
    turned[...] = jnp.zeros_like(turned)
    turned[0:tasks, :] = columns
    turned[tasks:tasks + 1, 0:tasks] = bias[...]
    across = turned[...].T
    bias_column = across[0:tasks, tasks:tasks + 1]
    small[0] = across[0:8, :]

    pl.semaphore_wait(barrier, nseq + ndp - 2)
    copies = small_start(0, "seq")

    def score(j):
        loads[j].wait()
        scores = lax.dot_general(
            weight[...], held[pl.ds(j * TOKENS, TOKENS), :], (((1,), (1,)), ((), ())),
            preferred_element_type=jnp.float32)
        for k in range(TOKENS // LANES):
            block = pl.ds(j * TOKENS + k * LANES, LANES)
            chosen, valid = onehot_of(block)
            predicted[:, block] = jnp.sum(
                jnp.where(chosen, scores[:, k * LANES:(k + 1) * LANES] + bias_column, 0.0),
                axis=0, keepdims=True)

    score(0)
    small[1] = small_finish(0, "seq", copies)
    copies = small_start(0, "dp")
    for j in range(1, tokens // TOKENS):
        score(j)
    turned[0:8, :] = small_finish(0, "dp", copies)

    across = turned[...].T
    counts, sums, squares = (across[0:tasks, k:k + 1] for k in range(3))
    floor_counts = jnp.maximum(counts, 1.0)
    means = sums / floor_counts
    spread = jnp.sqrt((squares - sums * means) / floor_counts + 0.1)
    means, spread = (jnp.broadcast_to(v, (tasks, LANES)) for v in (means, spread))
    gathered = jnp.zeros((tasks, LANES), jnp.float32)
    for block in blocks:
        chosen, valid = onehot_of(block)
        mean = jnp.sum(jnp.where(chosen, means, 0.0), axis=0, keepdims=True)
        scale = jnp.sum(jnp.where(chosen, spread, 0.0), axis=0, keepdims=True)
        target = (returns[:, block] - mean) / scale
        targets[:, block] = target
        slope = valid * jnp.clip(predicted[:, block] - target, -1.0, 1.0) / rollouts
        part = jnp.where(chosen, slope, 0.0)
        gathered = gathered + part
        coef[:, block] = part.astype(jnp.bfloat16)

    half = tiles // (streams * sizes["core"])

    def multiply(stream, which):
        first = stream * (tiles // streams) + which * half
        done = 0
        while done < half:
            now = min(32, half - done)
            start = pl.multiple_of((first + done) * (LANES // 8), LANES)
            product = jnp.dot(coef[...], held[:, pl.ds(start, now * (LANES // 8))],
                              preferred_element_type=jnp.float32)
            for b in range(now // 8):
                acc[pl.ds(first + done + b * 8, 8)] = product[:, b * LANES:(b + 1) * LANES].reshape(8, 8, LANES)
            done += now

    orders = [("core", "x", "y", "z"), ("core", "y", "x", "z")]

    class Stream:
        def __init__(self, index):
            self.index = index
            self.start = index * (tiles // streams)
            self.length = tiles // streams
            self.stage = 0
            self.path = []
            self.names = [n for n in orders[index % 2]]

        def scatter_start(self):
            name = self.names[self.stage]
            n, me = sizes[name], place[name]
            piece = self.length // n
            landing, send, recv = stage_scratch[3 * self.stage:3 * self.stage + 3]
            self.copies = []
            for r in range(1, n):
                self.copies.append(pltpu.make_async_remote_copy(
                    src_ref=acc.at[pl.ds(self.start + lax.rem(me + r, n) * piece, piece)],
                    dst_ref=landing.at[self.index, r - 1, pl.ds(0, piece)],
                    send_sem=send.at[0, self.index, r - 1], recv_sem=recv.at[0, self.index, r - 1],
                    device_id=peer(name, r), device_id_type=MESH))
                self.copies[-1].start()

        def scatter_finish(self, last):
            name = self.names[self.stage]
            n, me = sizes[name], place[name]
            piece = self.length // n
            landing = stage_scratch[3 * self.stage]
            self.path.append((self.start, piece))
            mine = pl.ds(self.start + me * piece, piece)
            total = acc[mine]
            for r, copy in enumerate(self.copies):
                copy.wait()
                total = total + landing[self.index, r, 0:piece]
            (whole if last else acc)[mine] = total
            self.start, self.length = self.start + me * piece, piece
            self.stage += 1

        def gather_start(self):
            self.stage -= 1
            name = self.names[self.stage]
            n, me = sizes[name], place[name]
            landing, send, recv = stage_scratch[3 * self.stage:3 * self.stage + 3]
            start, piece = self.path[self.stage]
            self.sent, self.due = [], []
            for r in range(1, n):
                for at, into in ((me, self.sent), (lax.rem(me + n - r, n), self.due)):
                    block = pl.ds(start + at * piece, piece)
                    into.append(pltpu.make_async_remote_copy(
                        src_ref=whole.at[block], dst_ref=whole.at[block],
                        send_sem=send.at[1, self.index, r - 1], recv_sem=recv.at[1, self.index, r - 1],
                        device_id=peer(name, r), device_id_type=MESH))
                self.sent[-1].start()

        def gather_finish(self):
            for sent, due in zip(self.sent, self.due):
                sent.wait_send()
                due.wait_recv()

    work = [Stream(i) for i in range(streams)]
    for stream in work:
        for r in range(1, sizes["core"]):
            multiply(stream.index, lax.rem(core + r, sizes["core"]))
        stream.scatter_start()
    for stream in work:
        multiply(stream.index, core)
        stream.scatter_finish(False)
        stream.scatter_start()

    turned[0:tasks, :] = jnp.where(lane == 0, jnp.sum(gathered, axis=1, keepdims=True), 0.0)
    small[2] = turned[...].T[0:8, :]
    copies = small_start(1, "seq")
    for stage in (1, 2):
        for stream in work:
            stream.scatter_finish(False)
            stream.scatter_start()
        if stage == 1:
            small[3] = small_finish(1, "seq", copies)
            copies = small_start(1, "dp")
    for stream in work:
        stream.scatter_finish(True)
        stream.gather_start()
    bias_grad[...] = small_finish(1, "dp", copies)[0:1, 0:tasks]
    for stage in range(3):
        for stream in work:
            stream.gather_finish()
            stream.gather_start()
    for stream in work:
        stream.gather_finish()
        first, count = stream.index * (tiles // streams) // 8, tiles // streams // 8
        for b in range(first, first + count):
            grad[:, b * LANES:(b + 1) * LANES] = whole[b * 8:(b + 1) * 8].reshape(tasks, LANES)


def solution(mesh):
    ndp, nseq = mesh.shape["dp"], mesh.shape["seq"]

    def on_device(hidden, value_weight, value_bias, returns, task_bins, loss_mask):
        width, tasks = value_weight.shape
        tokens = hidden.shape[0] * hidden.shape[1]
        rollouts = hidden.shape[0] * ndp
        tiles = width * tasks // (8 * LANES)
        sizes, streams = plan(ndp, nseq, tiles)
        f32 = jnp.float32
        stages = []
        length = tiles // streams
        for name in ("core", "y", "x", "z"):
            n = sizes[name]
            if name in ("y", "x"):
                n = max(sizes["y"], sizes["x"])
                piece = length // min(sizes["y"], sizes["x"])
                if name == "x":
                    piece = length
            else:
                piece = length // n
            stages += [
                pltpu.VMEM((streams, max(n - 1, 1), piece, 8, LANES), f32),
                pltpu.SemaphoreType.DMA((2, streams, max(n - 1, 1))),
                pltpu.SemaphoreType.DMA((2, streams, max(n - 1, 1))),
            ]
            length = length // sizes[name]
        vmem = pl.BlockSpec(memory_space=pltpu.VMEM)
        targets, grad, bias_grad = pl.pallas_call(
            functools.partial(kernel, ndp, nseq, rollouts, sizes, streams),
            out_shape=(
                jax.ShapeDtypeStruct((1, tokens), f32),
                jax.ShapeDtypeStruct((tasks, width), f32),
                jax.ShapeDtypeStruct((1, tasks), f32),
            ),
            in_specs=[pl.BlockSpec(memory_space=pl.ANY)] + [vmem] * 5,
            out_specs=(vmem, vmem, vmem),
            scratch_shapes=[
                pltpu.VMEM((tokens, width), jnp.bfloat16),
                pltpu.VMEM((tiles, 8, LANES), f32),
                pltpu.VMEM((tiles, 8, LANES), f32),
                pltpu.VMEM((tasks, tokens), jnp.bfloat16),
                pltpu.VMEM((1, tokens), f32),
                pltpu.VMEM((LANES, LANES), f32),
                pltpu.VMEM((4, 8, LANES), f32),
                pltpu.VMEM((2, max(nseq - 1, 1), 8, LANES), f32),
                pltpu.VMEM((2, max(ndp - 1, 1), 8, LANES), f32),
                pltpu.SemaphoreType.DMA((tokens // TOKENS,)),
                pltpu.SemaphoreType.DMA((2, nseq + ndp)),
                pltpu.SemaphoreType.DMA((2, nseq + ndp)),
            ] + stages,
            compiler_params=pltpu.CompilerParams(
                collective_id=0, has_side_effects=True, vmem_limit_bytes=56 * 1024 * 1024),
        )(hidden.reshape(tokens, width), value_weight.T, value_bias.reshape(1, tasks),
          returns.reshape(1, tokens), task_bins.reshape(1, tokens), loss_mask.reshape(1, tokens))
        return targets.reshape(returns.shape), grad.T, bias_grad.reshape(tasks)

    placed = (P("dp", "seq", None), P(), P(), P("dp", "seq"), P("dp", "seq"), P("dp", "seq"))
    return jax.shard_map(
        on_device, mesh=mesh, in_specs=placed, out_specs=(P("dp", "seq"), P(), P()), check_vma=False
    )
```

```python
import functools

import jax
import jax.numpy as jnp
from jax import lax
from jax.experimental import pallas as pl
from jax.experimental.pallas import tpu as pltpu
from jax.sharding import PartitionSpec as P

MESH = pl.DeviceIdType.MESH
LANES = 128
TOKENS = 512
AHEAD = 3


def split_in_two(n):
    return 2 if n % 2 == 0 else 1


def plan(ndp, nseq, tiles):
    core, x = split_in_two(nseq), split_in_two(ndp)
    sizes = {"core": core, "y": nseq // core, "x": x, "z": ndp // x}
    streams = 4
    while streams > 1 and (tiles % (streams * ndp * nseq) or tiles % (streams * core * 8)):
        streams //= 2
    return sizes, streams


def kernel(ndp, nseq, rollouts, sizes, streams, hidden, far_weight, far_bias, far_returns, far_bins, far_mask,
           targets, grad, bias_grad, *scratch):
    (weight, bias, returns, bins, mask, load_sem, held, acc, whole, coef, predicted, turned, small, small_in, row_in, hid_sem,
     small_send, small_recv) = scratch[:18]
    stage_scratch = scratch[18:]
    tasks, width = weight.shape
    tokens = hidden.shape[0]
    tiles = acc.shape[0]
    dp, seq = lax.axis_index("dp"), lax.axis_index("seq")
    core, y = lax.rem(seq, sizes["core"]), lax.div(seq, sizes["core"])
    x, z = lax.rem(dp, sizes["x"]), lax.div(dp, sizes["x"])

    barrier = pltpu.get_barrier_semaphore()
    for r in range(1, nseq):
        pl.semaphore_signal(barrier, inc=1, device_id={"seq": lax.rem(seq + r, nseq)}, device_id_type=MESH)
    for r in range(1, ndp):
        pl.semaphore_signal(barrier, inc=1, device_id={"dp": lax.rem(dp + r, ndp)}, device_id_type=MESH)

    early = [pltpu.make_async_copy(far, near, load_sem.at[k]) for k, (far, near) in enumerate(
        ((far_returns, returns), (far_bins, bins), (far_mask, mask), (far_bias, bias), (far_weight, weight)))]
    for copy in early:
        copy.start()
    loads = []
    for j in range(tokens // TOKENS):
        rows = pl.ds(j * TOKENS, TOKENS)
        loads.append(pltpu.make_async_copy(hidden.at[rows], held.at[rows], hid_sem.at[j]))
        loads[-1].start()

    def peer(name, r):
        n = sizes[name]
        if name == "core":
            return {"seq": y * n + lax.rem(core + r, n)}
        if name == "y":
            return {"seq": lax.rem(y + r, n) * sizes["core"] + core}
        if name == "x":
            return {"dp": z * n + lax.rem(x + r, n)}
        return {"dp": lax.rem(z + r, n) * sizes["x"] + x}

    place = {"core": core, "y": y, "x": x, "z": z}

    def small_start(k, axis):
        n, me = (nseq, seq) if axis == "seq" else (ndp, dp)
        landing = small_in if axis == "seq" else row_in
        base = 0 if axis == "seq" else nseq - 1
        copies = []
        for r in range(1, n):
            copies.append(pltpu.make_async_remote_copy(
                src_ref=small.at[2 * k + (axis == "dp")], dst_ref=landing.at[k, r - 1],
                send_sem=small_send.at[k, base + r - 1], recv_sem=small_recv.at[k, base + r - 1],
                device_id={axis: lax.rem(me + r, n)}, device_id_type=MESH))
            copies[-1].start()
        return copies

    def small_finish(k, axis, copies):
        landing = small_in if axis == "seq" else row_in
        total = small[2 * k + (axis == "dp")]
        for r, copy in enumerate(copies):
            copy.wait()
            total = total + landing[k, r]
        return total

    def onehot_of(block):
        chosen = bins[:, block] == lax.broadcasted_iota(jnp.int32, (tasks, LANES), 0)
        return chosen, mask[:, block].astype(jnp.float32)

    for copy in early[:4]:
        copy.wait()
    blocks = [pl.ds(k * LANES, LANES) for k in range(tokens // LANES)]
    counted = summed = squared = jnp.zeros((tasks, LANES), jnp.float32)
    for block in blocks:
        chosen, valid = onehot_of(block)
        value = returns[:, block]
        counted = counted + jnp.where(chosen, valid, 0.0)
        summed = summed + jnp.where(chosen, valid * value, 0.0)
        squared = squared + jnp.where(chosen, valid * value * value, 0.0)
    lane = lax.broadcasted_iota(jnp.int32, (tasks, LANES), 1)
    columns = jnp.zeros((tasks, LANES), jnp.float32)
    for k, part in enumerate((counted, summed, squared)):
        columns = jnp.where(lane == k, jnp.sum(part, axis=1, keepdims=True), columns)
    turned[...] = jnp.zeros_like(turned)
    turned[0:tasks, :] = columns
    turned[tasks:tasks + 1, 0:tasks] = bias[...]
    across = turned[...].T
    bias_column = across[0:tasks, tasks:tasks + 1]
    small[0] = across[0:8, :]

    def score(j):
        loads[j].wait()
        scores = lax.dot_general(
            weight[...], held[pl.ds(j * TOKENS, TOKENS), :], (((1,), (1,)), ((), ())),
            preferred_element_type=jnp.float32)
        for k in range(TOKENS // LANES):
            block = pl.ds(j * TOKENS + k * LANES, LANES)
            chosen, valid = onehot_of(block)
            predicted[:, block] = jnp.sum(
                jnp.where(chosen, scores[:, k * LANES:(k + 1) * LANES] + bias_column, 0.0),
                axis=0, keepdims=True)

    early[4].wait()
    pl.semaphore_wait(barrier, nseq + ndp - 2)
    copies = small_start(0, "seq")
    score(0)
    small[1] = small_finish(0, "seq", copies)
    copies = small_start(0, "dp")
    for j in range(1, tokens // TOKENS):
        score(j)
    turned[0:8, :] = small_finish(0, "dp", copies)

    across = turned[...].T
    counts, sums, squares = (across[0:tasks, k:k + 1] for k in range(3))
    floor_counts = jnp.maximum(counts, 1.0)
    means = sums / floor_counts
    spread = jnp.sqrt((squares - sums * means) / floor_counts + 0.1)
    means, spread = (jnp.broadcast_to(v, (tasks, LANES)) for v in (means, spread))
    gathered = jnp.zeros((tasks, LANES), jnp.float32)
    for block in blocks:
        chosen, valid = onehot_of(block)
        mean = jnp.sum(jnp.where(chosen, means, 0.0), axis=0, keepdims=True)
        scale = jnp.sum(jnp.where(chosen, spread, 0.0), axis=0, keepdims=True)
        target = (returns[:, block] - mean) / scale
        targets[:, block] = target
        slope = valid * jnp.clip(predicted[:, block] - target, -1.0, 1.0) / rollouts
        part = jnp.where(chosen, slope, 0.0)
        gathered = gathered + part
        coef[:, block] = part.astype(jnp.bfloat16)

    half = tiles // (streams * sizes["core"])

    def multiply(stream, which):
        first = stream * (tiles // streams) + which * half
        done = 0
        while done < half:
            now = min(32, half - done)
            start = pl.multiple_of((first + done) * (LANES // 8), LANES)
            product = jnp.dot(coef[...], held[:, pl.ds(start, now * (LANES // 8))],
                              preferred_element_type=jnp.float32)
            for b in range(now // 8):
                acc[pl.ds(first + done + b * 8, 8)] = product[:, b * LANES:(b + 1) * LANES].reshape(8, 8, LANES)
            done += now

    orders = [("core", "x", "y", "z"), ("core", "y", "x", "z")]

    class Stream:
        def __init__(self, index):
            self.index = index
            self.start = index * (tiles // streams)
            self.length = tiles // streams
            self.stage = 0
            self.path = []
            self.names = [n for n in orders[index % 2]]

        def scatter_start(self):
            name = self.names[self.stage]
            n, me = sizes[name], place[name]
            piece = self.length // n
            landing, send, recv = stage_scratch[3 * self.stage:3 * self.stage + 3]
            self.copies = []
            for r in range(1, n):
                self.copies.append(pltpu.make_async_remote_copy(
                    src_ref=acc.at[pl.ds(self.start + lax.rem(me + r, n) * piece, piece)],
                    dst_ref=landing.at[self.index, r - 1, pl.ds(0, piece)],
                    send_sem=send.at[0, self.index, r - 1], recv_sem=recv.at[0, self.index, r - 1],
                    device_id=peer(name, r), device_id_type=MESH))
                self.copies[-1].start()

        def scatter_finish(self, last):
            name = self.names[self.stage]
            n, me = sizes[name], place[name]
            piece = self.length // n
            landing = stage_scratch[3 * self.stage]
            self.path.append((self.start, piece))
            mine = pl.ds(self.start + me * piece, piece)
            total = acc[mine]
            for r, copy in enumerate(self.copies):
                copy.wait()
                total = total + landing[self.index, r, 0:piece]
            (whole if last else acc)[mine] = total
            self.start, self.length = self.start + me * piece, piece
            self.stage += 1

        def gather_start(self):
            self.stage -= 1
            name = self.names[self.stage]
            n, me = sizes[name], place[name]
            landing, send, recv = stage_scratch[3 * self.stage:3 * self.stage + 3]
            start, piece = self.path[self.stage]
            self.sent, self.due = [], []
            for r in range(1, n):
                for at, into in ((me, self.sent), (lax.rem(me + n - r, n), self.due)):
                    block = pl.ds(start + at * piece, piece)
                    into.append(pltpu.make_async_remote_copy(
                        src_ref=whole.at[block], dst_ref=whole.at[block],
                        send_sem=send.at[1, self.index, r - 1], recv_sem=recv.at[1, self.index, r - 1],
                        device_id=peer(name, r), device_id_type=MESH))
                self.sent[-1].start()

        def gather_finish(self):
            for sent, due in zip(self.sent, self.due):
                sent.wait_send()
                due.wait_recv()

    work = [Stream(i) for i in range(streams)]
    def send_off(stream):
        for r in range(1, sizes["core"]):
            multiply(stream.index, lax.rem(core + r, sizes["core"]))
        stream.scatter_start()

    ahead = min(AHEAD, streams)
    for stream in work[:ahead]:
        send_off(stream)
    for i, stream in enumerate(work):
        multiply(stream.index, core)
        if i + ahead < streams:
            send_off(work[i + ahead])
        stream.scatter_finish(False)
        stream.scatter_start()

    turned[0:tasks, :] = jnp.where(lane == 0, jnp.sum(gathered, axis=1, keepdims=True), 0.0)
    small[2] = turned[...].T[0:8, :]
    copies = small_start(1, "seq")
    for stage in (1, 2):
        for stream in work:
            stream.scatter_finish(False)
            stream.scatter_start()
        if stage == 1:
            small[3] = small_finish(1, "seq", copies)
            copies = small_start(1, "dp")
    for stream in work:
        stream.scatter_finish(True)
        stream.gather_start()
    bias_grad[...] = small_finish(1, "dp", copies)[0:1, 0:tasks]
    for stage in range(3):
        for stream in work:
            stream.gather_finish()
            stream.gather_start()
    for stream in work:
        stream.gather_finish()
        first, count = stream.index * (tiles // streams) // 8, tiles // streams // 8
        for b in range(first, first + count):
            grad[:, b * LANES:(b + 1) * LANES] = whole[b * 8:(b + 1) * 8].reshape(tasks, LANES)


def finish(targets, grad, bias_grad, targets_out, grad_out, bias_out, sem):
    copies = [
        pltpu.make_async_copy(grad, grad_out, sem.at[0]),
        pltpu.make_async_copy(targets, targets_out, sem.at[1]),
        pltpu.make_async_copy(bias_grad, bias_out, sem.at[2]),
    ]
    for copy in copies:
        copy.start()
    for copy in copies:
        copy.wait()


def solution(mesh):
    ndp, nseq = mesh.shape["dp"], mesh.shape["seq"]

    def on_device(hidden, value_weight, value_bias, returns, task_bins, loss_mask):
        width, tasks = value_weight.shape
        tokens = hidden.shape[0] * hidden.shape[1]
        rollouts = hidden.shape[0] * ndp
        tiles = width * tasks // (8 * LANES)
        sizes, streams = plan(ndp, nseq, tiles)
        f32 = jnp.float32
        stages = []
        length = tiles // streams
        for name in ("core", "y", "x", "z"):
            n = sizes[name]
            if name in ("y", "x"):
                n = max(sizes["y"], sizes["x"])
                piece = length // min(sizes["y"], sizes["x"])
                if name == "x":
                    piece = length
            else:
                piece = length // n
            stages += [
                pltpu.VMEM((streams, max(n - 1, 1), piece, 8, LANES), f32),
                pltpu.SemaphoreType.DMA((2, streams, max(n - 1, 1))),
                pltpu.SemaphoreType.DMA((2, streams, max(n - 1, 1))),
            ]
            length = length // sizes[name]
        vmem = pl.BlockSpec(memory_space=pltpu.VMEM)
        targets, grad, bias_grad = pl.pallas_call(
            functools.partial(kernel, ndp, nseq, rollouts, sizes, streams),
            out_shape=(
                pltpu.VMEM((1, tokens), f32),
                pltpu.VMEM((tasks, width), f32),
                pltpu.VMEM((1, tasks), f32),
            ),
            in_specs=[pl.BlockSpec(memory_space=pl.ANY)] * 6,
            out_specs=(vmem, vmem, vmem),
            scratch_shapes=[
                pltpu.VMEM((tasks, width), jnp.bfloat16),
                pltpu.VMEM((1, tasks), f32),
                pltpu.VMEM((1, tokens), f32),
                pltpu.VMEM((1, tokens), jnp.int32),
                pltpu.VMEM((1, tokens), jnp.int32),
                pltpu.SemaphoreType.DMA((5,)),
                pltpu.VMEM((tokens, width), jnp.bfloat16),
                pltpu.VMEM((tiles, 8, LANES), f32),
                pltpu.VMEM((tiles, 8, LANES), f32),
                pltpu.VMEM((tasks, tokens), jnp.bfloat16),
                pltpu.VMEM((1, tokens), f32),
                pltpu.VMEM((LANES, LANES), f32),
                pltpu.VMEM((4, 8, LANES), f32),
                pltpu.VMEM((2, max(nseq - 1, 1), 8, LANES), f32),
                pltpu.VMEM((2, max(ndp - 1, 1), 8, LANES), f32),
                pltpu.SemaphoreType.DMA((tokens // TOKENS,)),
                pltpu.SemaphoreType.DMA((2, nseq + ndp)),
                pltpu.SemaphoreType.DMA((2, nseq + ndp)),
            ] + stages,
            compiler_params=pltpu.CompilerParams(
                collective_id=0, has_side_effects=True, vmem_limit_bytes=62 * 1024 * 1024 + 512 * 1024),
        )(hidden.reshape(tokens, width), value_weight.T, value_bias.reshape(1, tasks),
          returns.reshape(1, tokens), task_bins.reshape(1, tokens), loss_mask.reshape(1, tokens))
        hbm = pl.BlockSpec(memory_space=pltpu.HBM)
        targets, grad, bias_grad = pl.pallas_call(
            finish,
            out_shape=(
                jax.ShapeDtypeStruct((1, tokens), f32),
                jax.ShapeDtypeStruct((tasks, width), f32),
                jax.ShapeDtypeStruct((1, tasks), f32),
            ),
            in_specs=[vmem] * 3,
            out_specs=(hbm, hbm, hbm),
            scratch_shapes=[pltpu.SemaphoreType.DMA((3,))],
        )(*(pltpu.with_memory_space_constraint(v, pltpu.VMEM) for v in (targets, grad, bias_grad)))
        return targets.reshape(returns.shape), grad.T, bias_grad.reshape(tasks)

    placed = (P("dp", "seq", None), P(), P(), P("dp", "seq"), P("dp", "seq"), P("dp", "seq"))
    return jax.shard_map(
        on_device, mesh=mesh, in_specs=placed, out_specs=(P("dp", "seq"), P(), P()), check_vma=False
    )
```
